32 devices in a mesh: dp: 8 (over z, y), mp: 2 (over core), fsdp: 2 (over x).
Axes of the slice: x: 2, y: 2, z: 4, core: 2. Of those that a mesh axis runs over, the one named last changes fastest.
Arguments:
- features: bfloat16 [5, 1024, 512], P(None, ('dp', 'fsdp')), may hold values from -6 to 6
- memory_bank: bfloat16 [512, 32, 1024], P(('dp', 'fsdp')), may hold values from -1 to 1
- memory_fill: int32 [512], P(('dp', 'fsdp')), may hold values from 0 to 32
- left_keys: bfloat16 [512, 64, 1024], P(('dp', 'fsdp'), None, 'mp'), may hold values from -400 to 400
- left_values: bfloat16 [512, 64, 1024], P(('dp', 'fsdp'), None, 'mp'), may hold values from -6 to 6
- left_length: int32 [512], P(('dp', 'fsdp')), may hold values from 0 to 64
- w_query: bfloat16 [1024, 1024], P('fsdp', 'mp'), may hold values from -0.1875 to 0.1875
- w_key: bfloat16 [1024, 1024], P('fsdp', 'mp'), may hold values from -0.1875 to 0.1875
- w_value: bfloat16 [1024, 1024], P('fsdp', 'mp'), may hold values from -0.1875 to 0.1875
- w_out: bfloat16 [1024, 1024], P('mp', 'fsdp'), may hold values from -0.1875 to 0.1875
- w_up: bfloat16 [1024, 4096], P('fsdp', 'mp'), may hold values from -0.1875 to 0.1875
- w_down: bfloat16 [4096, 1024], P('mp', 'fsdp'), may hold values from -0.09375 to 0.09375
- out_gain: float32 [1024], replicated, may hold values from 0.1 to 1.9
Outputs:
- layer_out: bfloat16 [512, 5, 1024], P(('dp', 'fsdp'))
- memory_next: bfloat16 [512, 1024], P(('dp', 'fsdp'))
- center_keys: bfloat16 [512, 4, 1024], P(('dp', 'fsdp'), None, 'mp')
- center_values: bfloat16 [512, 4, 1024], P(('dp', 'fsdp'), None, 'mp')
The draws below stay inside these ranges and needn't reach their ends.
All inputs are finite; a program needn't handle non-finite values.
Results may differ from the reference program's by a relative error of at most 0.0095.
Values may be sent and summed in bfloat16 or wider, within the bound.
A program may use at most 128 MiB of HBM per device.

```python
import jax
import jax.numpy as jnp
from jax import lax

D = 1024
H = 16
HD = 64
FF = 4096
MEM = 32
LEFT = 64
GROUP = 4
FRAMES = 5
STR_DEV = 32
STREAMS = 512


def draw_left_keys(key, part):
    base = jnp.clip(jax.random.normal(jax.random.fold_in(key, 11), (STREAMS, LEFT, D), jnp.float32), -6.0, 6.0)
    return base.astype(jnp.bfloat16)


def set_ends(entries, key, least, top_value):
    place = [jax.random.randint(jax.random.fold_in(key, axis), (), 0, length) for axis, length in enumerate(entries.shape)]
    main_axis = entries.shape.index(max(entries.shape))
    beside = place[:main_axis] + [(place[main_axis] + 1) % entries.shape[main_axis]] + place[main_axis + 1:]
    return entries.at[tuple(place)].set(least).at[tuple(beside)].set(top_value)


def raised(values, key, source, target, parts, factor):
    def block_of(dim):
        return (jnp.arange(values.shape[dim]) // (values.shape[dim] // parts)).reshape((-1,) + (1,) * (values.ndim - 1 - dim))

    one_side = jax.random.permutation(key, parts)[block_of(target)]
    second = (block_of(target) + parts // 2) % parts
    return jnp.where((block_of(source) == one_side) | (block_of(source) == second), factor * values, values)


def levels(own_key, extent, pieces, smallest, top_value):
    level = 1.0
    for position, shards_of in pieces:
        heights = jax.random.uniform(jax.random.fold_in(jax.random.fold_in(own_key, 6), position), (shards_of,), jnp.float32, smallest / len(pieces), top_value / len(pieces))
        level = level * jnp.repeat(jnp.exp(heights), extent[position] // shards_of).reshape((-1,) + (1,) * (len(extent) - 1 - position))
    return level


def normal_values(stream_key, dims, width, most, shards=(), held_as=jnp.bfloat16):
    values = jax.random.normal(stream_key, dims, jnp.float32) * width
    if len(shards) > 0:
        values = levels(stream_key, dims, shards, -0.22, 0.18) * values
    return jnp.clip(values, min=-most, max=most).astype(held_as)


def bell_draw_with(stream_key, shape, width, limit, cuts, heavy, kind=jnp.bfloat16):
    values = width * jax.random.normal(stream_key, shape, jnp.float32)
    if cuts:
        values = values * levels(stream_key, shape, cuts, -0.22, 0.18)
    return jnp.clip(raised(values, jax.random.fold_in(stream_key, 3), *heavy), -limit, limit).astype(kind)


def setup_inputs(seed: int = 0) -> dict:
    streams_of = jax.random.split(jax.random.key(seed), 14)
    features = bell_draw_with(streams_of[0], (FRAMES, D, STREAMS), 1.0, 6.0, ((1, 16),), (1, 2, 16, 2.0))
    memory_bank = jnp.clip(jax.random.uniform(streams_of[1], (STREAMS, MEM, D), jnp.float32, -1.0, 1.0) * levels(streams_of[1], (STREAMS, MEM, D), ((0, 16),), -0.4, 0.0), -1.0, 1.0).astype(jnp.bfloat16)
    memory_fill = set_ends(jax.random.randint(streams_of[2], (STREAMS,), 0, MEM + 1), jax.random.fold_in(streams_of[2], 1), 0, MEM).astype(jnp.int32)
    left_keys = draw_left_keys(jax.random.fold_in(streams_of[13], 71), 0)
    left_values = normal_values(streams_of[4], (STREAMS, LEFT, D), 1.0, 6.0, ((0, 16), (2, 2)))
    left_length = set_ends(jax.random.randint(streams_of[5], (STREAMS,), 0, LEFT + 1), jax.random.fold_in(streams_of[5], 1), 0, LEFT).astype(jnp.int32)
    w_query = normal_values(streams_of[6], (D, D), D ** -0.5, 0.1875, ((0, 2), (1, 2)))
    w_key = normal_values(streams_of[7], (D, D), D ** -0.5, 0.1875, ((0, 2), (1, 2)))
    w_value = normal_values(streams_of[8], (D, D), D ** -0.5, 0.1875, ((0, 2), (1, 2)))
    w_out = normal_values(streams_of[9], (D, D), D ** -0.5, 0.1875, ((0, 2), (1, 2)))
    w_up = normal_values(streams_of[10], (D, FF), D ** -0.5, 0.1875, ((0, 2), (1, 2)))
    w_down = normal_values(streams_of[11], (FF, D), FF ** -0.5, 0.09375, ((0, 2), (1, 2)))
    out_gain = jnp.clip(1.0 + 0.18 * jax.random.normal(streams_of[12], (D,), jnp.float32), 0.1, 1.9)
    return {"features": features, "memory_bank": memory_bank, "memory_fill": memory_fill, "left_keys": left_keys, "left_values": left_values, "left_length": left_length, "w_query": w_query, "w_key": w_key, "w_value": w_value, "w_out": w_out, "w_up": w_up, "w_down": w_down, "out_gain": out_gain}


epsilon = 1e-05
masked_score = -1e+30

def normalize(values):
    values = values.astype(jnp.float32)
    average = lax.optimization_barrier(jnp.mean(values, axis=-1, keepdims=True))
    centred = values - average
    variance = lax.optimization_barrier(jnp.mean(centred * centred, axis=-1, keepdims=True))
    return centred * lax.rsqrt(variance + epsilon)

def visible_masks(fill, length, mem_slots, left_slots, query_count):
    mem_ok = jnp.arange(mem_slots, dtype=jnp.int32)[None, :] >= (mem_slots - fill)[:, None]
    not_summary = jnp.arange(query_count, dtype=jnp.int32) < query_count - 1
    mem_mask = mem_ok[:, None, None, :] & not_summary[None, None, :, None]
    left_ok = jnp.arange(left_slots, dtype=jnp.int32)[None, :] >= (left_slots - length)[:, None]
    left_mask = left_ok[:, None, None, :] & (not_summary[None, None, :, None] | True)
    return (mem_mask, left_mask)

def reference(features, memory_bank, memory_fill, left_keys, left_values, left_length, w_query, w_key, w_value, w_out, w_up, w_down, out_gain):
    streams = features.shape[2]
    inputs = jnp.transpose(features, (2, 0, 1))
    normed = normalize(inputs).astype(jnp.bfloat16)
    summary = lax.optimization_barrier(jnp.mean(normed[:, :GROUP, :].astype(jnp.float32), axis=1)).astype(jnp.bfloat16)
    query_rows = jnp.concatenate([normed, summary[:, None, :]], axis=1).reshape(-1, D)
    query_proj = jnp.dot(query_rows, w_query, preferred_element_type=jnp.float32).astype(jnp.bfloat16)
    group_rows = normed.reshape(-1, D)
    group_keys = jnp.dot(group_rows, w_key, preferred_element_type=jnp.float32).astype(jnp.bfloat16)
    group_values = jnp.dot(group_rows, w_value, preferred_element_type=jnp.float32).astype(jnp.bfloat16)
    blocks = streams // STR_DEV
    scale = HD ** (-0.5)

    def split(array):
        return array.reshape((blocks, STR_DEV) + array.shape[1:])

    def attend(operands):
        query_blk, ckey_blk, cval_blk, memory_blk, lkey_blk, lval_blk, fill_blk, length_blk = operands
        memory_rows = memory_blk.reshape(-1, D)
        mem_keys = jnp.dot(memory_rows, w_key, preferred_element_type=jnp.float32).astype(jnp.bfloat16)
        mem_values = jnp.dot(memory_rows, w_value, preferred_element_type=jnp.float32).astype(jnp.bfloat16)
        query_h = query_blk.reshape(STR_DEV, FRAMES + 1, H, HD).astype(jnp.float32)
        mkey_h = mem_keys.reshape(STR_DEV, MEM, H, HD).astype(jnp.float32)
        mval_h = mem_values.reshape(STR_DEV, MEM, H, HD).astype(jnp.float32)
        lkey_h = lkey_blk.reshape(STR_DEV, LEFT, H, HD).astype(jnp.float32)
        lval_h = lval_blk.reshape(STR_DEV, LEFT, H, HD).astype(jnp.float32)
        ckey_h = ckey_blk.reshape(STR_DEV, FRAMES, H, HD).astype(jnp.float32)
        cval_h = cval_blk.reshape(STR_DEV, FRAMES, H, HD).astype(jnp.float32)
        mem_mask, left_mask = visible_masks(fill_blk, length_blk, MEM, LEFT, FRAMES + 1)
        score_mem = jnp.einsum('sqhd,skhd->shqk', query_h, mkey_h) * scale
        score_left = jnp.einsum('sqhd,skhd->shqk', query_h, lkey_h) * scale
        score_group = jnp.einsum('sqhd,skhd->shqk', query_h, ckey_h) * scale
        score_mem = jnp.where(mem_mask, score_mem, masked_score)
        score_left = jnp.where(left_mask, score_left, masked_score)
        top = jnp.maximum(jnp.maximum(lax.optimization_barrier(jnp.max(score_mem, axis=-1, keepdims=True)), lax.optimization_barrier(jnp.max(score_left, axis=-1, keepdims=True))), lax.optimization_barrier(jnp.max(score_group, axis=-1, keepdims=True)))
        exp_mem = jnp.exp(score_mem - top)
        exp_left = jnp.exp(score_left - top)
        exp_group = jnp.exp(score_group - top)
        totals = lax.optimization_barrier(jnp.sum(exp_mem, axis=-1, keepdims=True)) + lax.optimization_barrier(jnp.sum(exp_left, axis=-1, keepdims=True)) + lax.optimization_barrier(jnp.sum(exp_group, axis=-1, keepdims=True))
        prob_mem = (exp_mem / totals).astype(jnp.bfloat16).astype(jnp.float32)
        prob_left = (exp_left / totals).astype(jnp.bfloat16).astype(jnp.float32)
        prob_group = (exp_group / totals).astype(jnp.bfloat16).astype(jnp.float32)
        attended = jnp.einsum('shqk,skhd->sqhd', prob_mem, mval_h) + jnp.einsum('shqk,skhd->sqhd', prob_left, lval_h) + jnp.einsum('shqk,skhd->sqhd', prob_group, cval_h)
        return attended.astype(jnp.bfloat16).reshape(STR_DEV, FRAMES + 1, D)
    attended = lax.map(attend, (split(query_proj.reshape(streams, (FRAMES + 1) * D)), split(group_keys.reshape(streams, FRAMES * D)), split(group_values.reshape(streams, FRAMES * D)), split(memory_bank), split(left_keys), split(left_values), split(memory_fill), split(left_length)))
    attended = attended.reshape(-1, D)
    attn_out = jnp.dot(attended, w_out, preferred_element_type=jnp.float32).reshape(streams, FRAMES + 1, D)
    memory_next = jnp.tanh(attn_out[:, FRAMES, :]).astype(jnp.bfloat16)
    hidden_state = inputs.astype(jnp.float32) + attn_out[:, :FRAMES, :]
    h_norm = normalize(hidden_state).astype(jnp.bfloat16).reshape(-1, D)
    up_proj = jax.nn.gelu(jnp.dot(h_norm, w_up, preferred_element_type=jnp.float32), approximate=True).astype(jnp.bfloat16)
    down_proj = jnp.dot(up_proj, w_down, preferred_element_type=jnp.float32)
    layer_out = (normalize(hidden_state.reshape(-1, D) + down_proj) * out_gain.astype(jnp.float32)).astype(jnp.bfloat16).reshape(streams, FRAMES, D)
    center_keys = group_keys.reshape(streams, FRAMES, D)[:, :GROUP, :]
    center_values = group_values.reshape(streams, FRAMES, D)[:, :GROUP, :]
    return (layer_out, memory_next, center_keys, center_values)
```

```python
import functools

import jax
import jax.numpy as jnp
from jax import lax
from jax.experimental import pallas as pl
from jax.experimental.pallas import tpu as pltpu
from jax.sharding import PartitionSpec as P

HD = 64
GROUP = 4
ROWS = 8
KEYS = 128
LEAD = 3

epsilon = 1e-05
masked_score = -1e30
MESH = pl.DeviceIdType.MESH
bf16 = jnp.bfloat16
f32 = jnp.float32


def normalize(values):
    average = jnp.mean(values, axis=-1, keepdims=True)
    centred = values - average
    variance = jnp.mean(centred * centred, axis=-1, keepdims=True)
    return centred * lax.rsqrt(variance + epsilon)


def matmul(left, right):
    return jnp.dot(left, right, preferred_element_type=f32)


def body(
    frames,
    mem_slots,
    left_slots,
    packed,
    f_hbm,
    fill_hbm,
    length_hbm,
    gain_hbm,
    mem_hbm,
    lk_hbm,
    lv_hbm,
    wq_hbm,
    wk_hbm,
    wv_hbm,
    wo_hbm,
    wu_hbm,
    wd_hbm,
    out_ref,
    mnext_ref,
    ck_ref,
    cv_ref,
    f_ref,
    fill_ref,
    length_ref,
    gain_ref,
    x_ref,
    outbox,
    inbox,
    far,
    own,
    mem_v,
    lk_v,
    lv_v,
    mk,
    mv,
    gk,
    gv,
    qs,
    rows_v,
    att,
    hid,
    hn,
    hn_far,
    act,
    act_far,
    dacc,
    dacc_far,
    part,
    peer,
    stage_out,
    stage_in,
    send_sem,
    recv_sem,
    psend_sem,
    precv_sem,
    load_sem,
    fsend_sem,
    frecv_sem,
    gsend_sem,
    grecv_sem,
    hello,
):
    d = lax.axis_index("dp")
    m = lax.axis_index("mp")
    f = lax.axis_index("fsdp")
    total, width = rows_v.shape
    streams = total // ROWS
    count = frames * streams
    half = count // 2
    n_blocks, depth, cols = far.shape
    n_ff = (n_blocks - 4) // 2
    n_hid = n_ff * cols
    quarter = depth // 4
    c1 = quarter // 4
    c2 = (quarter - c1) // 2
    ybit = lax.rem(d, 2)
    zbit = lax.rem(lax.div(d, 2), 2)
    p = lax.rem(d, 4)
    py = p + 1 - 2 * ybit
    pz = p + 2 - 4 * zbit
    pd = 3 - p
    xdev = (d, m, 1 - f)
    ydev = (d + 1 - 2 * ybit, m, f)
    zdev = (d + 2 - 4 * zbit, m, f)
    mdev = (d, 1 - m, f)

    def own_hbm(b, start, size, side):
        r = pl.ds(pl.multiple_of(start, 16), size)
        if b < 4:
            return (wk_hbm, wv_hbm, wq_hbm, wo_hbm)[b].at[r, :]
        j = (b - 4) // 2
        first = side * n_hid + j * cols
        if b % 2 == 0:
            return wu_hbm.at[r, pl.ds(pl.multiple_of(first, 128), cols)]
        return wd_hbm.at[pl.ds(pl.multiple_of(start + first, 16), size), :]

    def piece(b, start, size):
        return far.at[b, pl.ds(pl.multiple_of(start, 16), size), :]

    sends = []

    def push(src, dst, s_sem, r_sem, dev):
        copy = pltpu.make_async_remote_copy(
            src_ref=src,
            dst_ref=dst,
            send_sem=s_sem,
            recv_sem=r_sem,
            device_id=dev,
            device_id_type=MESH,
        )
        copy.start()
        sends.append(copy)
        return copy

    def landed(ref, s_sem, r_sem):
        pltpu.make_async_remote_copy(
            src_ref=ref,
            dst_ref=ref,
            send_sem=s_sem,
            recv_sem=r_sem,
            device_id=xdev,
            device_id_type=MESH,
        ).wait_recv()

    def send(src, b, start, size, dev, kind):
        push(src, piece(b, start, size), send_sem.at[b, kind], recv_sem.at[b, kind], dev)

    def arrived(b, start, size, kind):
        landed(piece(b, start, size), send_sem.at[b, kind], recv_sem.at[b, kind])

    def load(src, dst, i):
        copy = pltpu.make_async_copy(src, dst, load_sem.at[i])
        copy.start()
        return copy

    peers = inbox.shape[0] if packed else 0
    n_fsdp = lax.axis_size("fsdp")
    me = d * n_fsdp + f

    def place(offset):
        return lax.rem(me + offset, peers)

    def device_of(index):
        return (lax.div(index, n_fsdp), m, lax.rem(index, n_fsdp))

    barrier = pltpu.get_barrier_semaphore()
    greeted = [xdev, ydev, zdev, mdev]
    if packed:
        wbit = lax.rem(lax.div(d, 4), 2)
        greeted.append((d + 4 - 8 * wbit, m, f))
    for dev in greeted:
        pl.semaphore_signal(barrier, inc=1, device_id=dev, device_id_type=MESH)

    f_load = load(f_hbm, f_ref if packed else x_ref, n_blocks + 3)
    small_loads = [
        load(fill_hbm, fill_ref, n_blocks + 4),
        load(length_hbm, length_ref, n_blocks + 5),
        load(gain_hbm, gain_ref, n_blocks + 6),
    ]

    if packed:
        f_load.wait()
        pairs = outbox.shape[1]
        for k in range(pairs):
            low = f_ref[2 * k].astype(f32)
            high = f_ref[min(2 * k + 1, frames - 1)].astype(f32)
            turned = jnp.concatenate([low, high], axis=0).T.astype(bf16)
            outbox[:, k] = turned.reshape(peers, streams, turned.shape[1])

    with jax.named_scope("barwait"):
        pl.semaphore_wait(barrier, len(greeted))

    def send_quarter(b):
        send(own_hbm(b, p * quarter, quarter, 1 - f), b, p * quarter, quarter, xdev, 0)

    def send_rest(b):
        send(own_hbm(b, pd * quarter, c1, 1 - f), b, pd * quarter, c1, xdev, 1)

    def send_own(b):
        if b >= n_blocks:
            return
        send_quarter(b)
        send_rest(b)

    send_quarter(0)
    share = streams // 2

    def slot(box, i, side):
        return box.at[i, :, pl.ds(pl.multiple_of(side * share, 16), share), :]

    if packed:
        for i, dev in enumerate((zdev, ydev, xdev)):
            with jax.named_scope("hello%d" % i):
                pl.semaphore_signal(hello.at[i], inc=1, device_id=dev, device_id_type=MESH)
                pl.semaphore_wait(hello.at[i], 1)
        for o in range(1, peers):
            push(
                slot(outbox, place(o), m),
                slot(inbox, me, m),
                fsend_sem.at[o],
                frecv_sem.at[o],
                device_of(place(o)),
            )
    send_rest(0)
    for b in range(1, LEAD):
        send_own(b)

    loads = [load(own_hbm(b, 0, depth, f), own.at[b], b) for b in range(n_blocks)]
    mem_load = load(mem_hbm, mem_v, n_blocks)
    lk_load = load(lk_hbm, lk_v, n_blocks + 1)
    lv_load = load(lv_hbm, lv_v, n_blocks + 2)

    def pass_quarter(b):
        if b >= n_blocks:
            return
        arrived(b, p * quarter, quarter, 0)
        send_own(b + LEAD)
        src = piece(b, p * quarter, quarter)
        send(src, b, p * quarter, quarter, ydev, 2)
        send(src, b, p * quarter, quarter, zdev, 3)

    def pass_diagonal(b):
        if b >= n_blocks:
            return
        at_y = pz * quarter + c1
        arrived(b, pz * quarter, quarter, 3)
        send(piece(b, at_y, c2), b, at_y, c2, ydev, 4)
        at_z = py * quarter + c1 + c2
        arrived(b, py * quarter, quarter, 2)
        send(piece(b, at_z, c2), b, at_z, c2, zdev, 5)

    def complete(b):
        loads[b].wait()
        arrived(b, pd * quarter, c1, 1)
        arrived(b, pd * quarter + c1, c2, 4)
        arrived(b, pd * quarter + c1 + c2, c2, 5)

    def pump(b):
        pass_diagonal(b - 2)
        pass_quarter(b)

    mine = pl.ds(pl.multiple_of(f * depth, 128), depth)
    other = pl.ds(pl.multiple_of((1 - f) * depth, 128), depth)

    with jax.named_scope("r01"):
        pass_quarter(0)
        pass_quarter(1)

    if packed:
        inbox[pl.ds(me, 1)] = outbox[pl.ds(me, 1)]
        with jax.named_scope("fwait"):
            for o in range(1, peers):
                ref = slot(inbox, lax.rem(me + peers - o, peers), m)
                landed(ref, fsend_sem.at[o], frecv_sem.at[o])
                push(ref, ref, gsend_sem.at[o], grecv_sem.at[o], mdev)
        with jax.named_scope("gwait"):
            for o in range(1, peers):
                ref = slot(inbox, lax.rem(me + peers - o, peers), 1 - m)
                landed(ref, gsend_sem.at[o], grecv_sem.at[o])
        lane_half = inbox.shape[3] // 2
        for t in range(frames):
            k, side = t // 2, t % 2
            lanes = slice(side * lane_half, side * lane_half + lane_half)
            x_ref[t * streams : (t + 1) * streams, :] = jnp.concatenate(
                [inbox[i, k][:, lanes] for i in range(peers)], axis=1
            )
    else:
        f_load.wait()

    with jax.named_scope("norm"):
        summed = None
        major = []
        for t in range(frames):
            n = normalize(x_ref[t * streams : (t + 1) * streams, :].astype(f32)).astype(bf16)
            major.append(n)
            if t < GROUP:
                summed = n.astype(f32) if t == 0 else summed + n.astype(f32)
        major.append((summed * (1.0 / GROUP)).astype(bf16))
        major = jnp.concatenate(major, axis=0)
        packed_rows = count + streams
        r_id = lax.broadcasted_iota(jnp.int32, (total, packed_rows), 0)
        c_id = lax.broadcasted_iota(jnp.int32, (total, packed_rows), 1)
        frame_id = r_id % ROWS
        target = jnp.where(frame_id <= frames, frame_id * streams + r_id // ROWS, -1)
        spread_rows = jnp.where(target == c_id, 1.0, 0.0).astype(bf16)
        rows_v[...] = matmul(spread_rows, major).astype(bf16)

    with jax.named_scope("pump2"):
        pump(2)
        mem_load.wait()

    def project(b):
        with jax.named_scope("c%d" % b):
            complete(b)
        sums = matmul(rows_v[:, mine], own[b]) + matmul(rows_v[:, other], far[b])
        return sums.astype(bf16)

    def project_memory(b, target):
        step = 256

        @pl.loop(0, mem_v.shape[0] // step)
        def _(i):
            r = pl.ds(pl.multiple_of(i * step, step), step)
            sums = matmul(mem_v[r, mine], own[b]) + matmul(mem_v[r, other], far[b])
            target[r, :] = sums.astype(bf16)

    keys = project(0).astype(f32)
    gk[...] = keys
    ck_ref[...] = keys.reshape(streams, ROWS, cols)[:, :GROUP].astype(bf16)
    project_memory(0, mk)
    with jax.named_scope("pump3"):
        pump(3)
    vals = project(1).astype(f32)
    gv[...] = vals
    cv_ref[...] = vals.reshape(streams, ROWS, cols)[:, :GROUP].astype(bf16)
    project_memory(1, mv)
    with jax.named_scope("pump4"):
        pump(4)
    qs[...] = project(2).astype(f32)
    for copy in [lk_load, lv_load] + small_loads:
        copy.wait()

    heads = cols // HD
    lanes3 = lax.broadcasted_iota(jnp.int32, (heads, ROWS, cols), 2)
    head3 = lax.broadcasted_iota(jnp.int32, (heads, ROWS, cols), 0)
    head_mask = jnp.where(lanes3 // HD == head3, 1.0, 0.0).astype(f32)
    row2 = lax.broadcasted_iota(jnp.int32, (heads * ROWS, KEYS), 0)
    lane2 = lax.broadcasted_iota(jnp.int32, (heads * ROWS, KEYS), 1)
    excluded = jnp.where((row2 % ROWS == frames) & (lane2 < mem_slots), -1.0, 0.0).astype(f32)
    lane1 = lax.broadcasted_iota(jnp.int32, (1, KEYS), 1)
    left_end = mem_slots + left_slots
    pad8 = jnp.zeros((16 - ROWS, cols), f32)
    pad = jnp.zeros((KEYS - mem_slots - left_slots - 16, cols), bf16)
    scale = HD ** (-0.5)

    def gather_rows(mem_part, left_part, group_part, s):
        return jnp.concatenate(
            [
                mem_part[pl.ds(pl.multiple_of(s * mem_slots, mem_slots), mem_slots), :],
                left_part[s],
                jnp.concatenate(
                    [group_part[pl.ds(pl.multiple_of(s * ROWS, ROWS), ROWS), :], pad8], axis=0
                ).astype(bf16),
                pad,
            ],
            axis=0,
        )

    def attend(s):
        r = pl.ds(pl.multiple_of(s * ROWS, ROWS), ROWS)
        spread = (qs[r, :][None] * head_mask).reshape(heads * ROWS, cols).astype(bf16)
        k = gather_rows(mk, lk_v, gk, s)
        scores = (
            lax.dot_general(spread, k, (((1,), (1,)), ((), ())), preferred_element_type=f32) * scale
        )
        first_mem = mem_slots - fill_ref[s]
        first_left = left_end - length_ref[s]
        first = jnp.where(lane1 < mem_slots, first_mem, first_left)
        first = jnp.where(lane1 < left_end, first, 0)
        hide1 = (lane1 < first) | (lane1 >= left_end + frames)
        hide = jnp.where(hide1, -1.0, 0.0) + excluded
        scores = jnp.where(hide < 0.0, masked_score, scores)
        top = jnp.max(scores, axis=-1, keepdims=True)
        e = jnp.exp(scores - top)
        probs = (e / jnp.sum(e, axis=-1, keepdims=True)).astype(bf16)
        v = gather_rows(mv, lv_v, gv, s)
        o = matmul(probs, v).reshape(heads, ROWS, cols) * head_mask
        att[r, :] = jnp.sum(o, axis=0)

    chunks = 4
    per_chunk = streams // chunks
    unroll = 4
    for c in range(chunks):
        with jax.named_scope("att%d" % c):

            @pl.loop(0, per_chunk // unroll)
            def _(i):
                for u in range(unroll):
                    attend(c * per_chunk + i * unroll + u)

        with jax.named_scope("apump%d" % c):
            if c != 2:
                pump(5 + min(c, 2))

    with jax.named_scope("c3"):
        complete(3)
    with jax.named_scope("oproj"):
        r_id = lax.broadcasted_iota(jnp.int32, (packed_rows, total), 0)
        c_id = lax.broadcasted_iota(jnp.int32, (packed_rows, total), 1)
        pick = (r_id % streams) * ROWS + r_id // streams
        gather = jnp.where(pick == c_id, 1.0, 0.0).astype(bf16)
        attended = matmul(gather, att[...].astype(bf16)).astype(bf16)
        part[:, mine] = matmul(attended, own[3]).astype(bf16)
        part[:, other] = matmul(attended, far[3]).astype(bf16)
    push(part, peer, psend_sem.at[0], precv_sem.at[0], mdev)
    with jax.named_scope("d6"):
        for b in range(6, n_blocks - 1):
            pass_diagonal(b)
            pass_quarter(b + 2)
    with jax.named_scope("ex0"):
        landed(peer, psend_sem.at[0], precv_sem.at[0])

    my_half = pl.multiple_of(m * half, 16)
    its_half = pl.multiple_of((1 - m) * half, 16)

    def residual(start):
        r = pl.ds(start, half)
        h = x_ref[r, :].astype(f32) + (part[r, :].astype(f32) + peer[r, :].astype(f32))
        hid[r, :] = h
        hn[r, :] = normalize(h).astype(bf16)

    with jax.named_scope("hid"):
        residual(my_half)
        rows_mine = pl.ds(my_half, half)
        rows_its = pl.ds(its_half, half)
        push(
            hn.at[rows_mine, :], hn_far.at[rows_mine, :], psend_sem.at[1], precv_sem.at[1], xdev
        )
        residual(its_half)
        s = slice(count, packed_rows)
        mnext_ref[...] = jnp.tanh(part[s, :].astype(f32) + peer[s, :].astype(f32)).astype(bf16)

    def up(rows, target, j):
        sums = matmul(rows[:, mine], own[4 + 2 * j]) + matmul(rows[:, other], far[4 + 2 * j])
        target[:, j * cols : (j + 1) * cols] = jax.nn.gelu(sums, approximate=True).astype(bf16)

    def down(rows, target, j):
        hidden = rows[:, j * cols : (j + 1) * cols]
        for sel, weights in ((mine, own), (other, far)):
            sums = matmul(hidden, weights[5 + 2 * j])
            target[:, sel] = sums if j == 0 else target[:, sel] + sums

    for j in range(n_ff):
        with jax.named_scope("c_up%d" % j):
            complete(4 + 2 * j)
        with jax.named_scope("up%d" % j):
            up(hn, act, j)
        if j < n_ff - 1:
            with jax.named_scope("c_dn%d" % j):
                complete(5 + 2 * j)
            with jax.named_scope("dn%d" % j):
                down(act, dacc, j)
        if j == 0:
            with jax.named_scope("d7"):
                pass_diagonal(n_blocks - 1)
    with jax.named_scope("hnwait"):
        landed(hn_far.at[rows_mine, :], psend_sem.at[1], precv_sem.at[1])
        push(
            hn_far.at[rows_mine, :],
            hn_far.at[rows_mine, :],
            psend_sem.at[2],
            precv_sem.at[2],
            mdev,
        )
        landed(hn_far.at[rows_its, :], psend_sem.at[2], precv_sem.at[2])
    with jax.named_scope("farup"):
        for j in range(n_ff):
            up(hn_far, act_far, j)
    with jax.named_scope("c7"):
        complete(n_blocks - 1)
    with jax.named_scope("fardn"):
        for j in range(n_ff):
            down(act_far, dacc_far, j)
        stage_out[0] = dacc_far[rows_its, :].astype(bf16)
    push(stage_out.at[0], stage_in.at[0], psend_sem.at[3], precv_sem.at[3], mdev)
    with jax.named_scope("dnlast"):
        down(act, dacc, n_ff - 1)
        stage_out[1] = dacc[rows_its, :].astype(bf16)
    push(stage_out.at[1], stage_in.at[1], psend_sem.at[4], precv_sem.at[4], mdev)
    with jax.named_scope("xsum"):
        landed(stage_in.at[0], psend_sem.at[3], precv_sem.at[3])
        stage_out[2] = (dacc_far[rows_mine, :] + stage_in[0].astype(f32)).astype(bf16)
    push(stage_out.at[2], stage_in.at[2], psend_sem.at[5], precv_sem.at[5], xdev)
    with jax.named_scope("ownsum"):
        landed(stage_in.at[1], psend_sem.at[4], precv_sem.at[4])
        hid[rows_mine, :] = hid[rows_mine, :] + (dacc[rows_mine, :] + stage_in[1].astype(f32))
    with jax.named_scope("xwait"):
        landed(stage_in.at[2], psend_sem.at[5], precv_sem.at[5])
    with jax.named_scope("final"):
        y = hid[rows_mine, :] + stage_in[2].astype(f32)
        y = (normalize(y) * gain_ref[...]).astype(bf16)
        stage_out[3] = y
        out_ref[rows_mine, :] = y
    push(stage_out.at[3], stage_in.at[3], psend_sem.at[6], precv_sem.at[6], mdev)
    with jax.named_scope("lastwait"):
        landed(stage_in.at[3], psend_sem.at[6], precv_sem.at[6])
        out_ref[rows_its, :] = stage_in[3]

    with jax.named_scope("sendwait"):
        for copy in sends:
            copy.wait_send()


def finish(rows_ref, mem_ref, keys_ref, vals_ref, out_ref, mnext_ref, ck_ref, cv_ref):
    out_ref[...] = rows_ref[...]
    mnext_ref[...] = mem_ref[...]
    ck_ref[...] = keys_ref[...]
    cv_ref[...] = vals_ref[...]


def shards(
    features,
    memory_bank,
    memory_fill,
    left_keys,
    left_values,
    left_length,
    w_query,
    w_key,
    w_value,
    w_out,
    w_up,
    w_down,
    out_gain,
):
    frames, width_dev, all_streams = features.shape
    streams, mem_slots, width = memory_bank.shape
    left_slots = left_keys.shape[1]
    depth, cols = w_query.shape
    n_dp = lax.axis_size("dp")
    n_fsdp = lax.axis_size("fsdp")
    n_ff = w_up.shape[1] // (n_fsdp * cols)
    n_blocks = 4 + 2 * n_ff
    total = streams * ROWS
    count = frames * streams
    peers = n_dp * n_fsdp
    packed = 2 * width_dev == KEYS and streams % 32 == 0 and n_dp == 8 and n_fsdp == 2
    if packed:
        feed = features
    else:
        flat = features.reshape(frames * width_dev, all_streams)
        got = lax.all_to_all(flat, ("dp", "fsdp"), split_axis=1, concat_axis=0, tiled=True)
        got = got.reshape(peers, frames, width_dev, streams)
        feed = jnp.transpose(got, (1, 3, 0, 2)).reshape(count, width)
    slots = (peers, (frames + 1) // 2, streams, KEYS) if packed else (1, 1, 32, KEYS)
    vmem = pl.BlockSpec(memory_space=pltpu.VMEM)
    hbm = pl.BlockSpec(memory_space=pl.ANY)
    results = (
        ((count, width), bf16),
        ((streams, width), bf16),
        ((streams, GROUP, cols), bf16),
        ((streams, GROUP, cols), bf16),
    )
    middle = pl.pallas_call(
        functools.partial(body, frames, mem_slots, left_slots, packed),
        out_shape=tuple(jax.ShapeDtypeStruct(*r) for r in results),
        in_specs=[hbm] * 13,
        out_specs=(vmem,) * 4,
        scratch_shapes=[
            pltpu.VMEM(features.shape if packed else (1, 16, KEYS), bf16),
            pltpu.SMEM((streams,), jnp.int32),
            pltpu.SMEM((streams,), jnp.int32),
            pltpu.VMEM((1, width), f32),
            pltpu.VMEM((count, width), bf16),
            pltpu.VMEM(slots, bf16),
            pltpu.VMEM(slots, bf16),
            pltpu.VMEM((n_blocks, depth, cols), bf16),
            pltpu.VMEM((n_blocks, depth, cols), bf16),
            pltpu.VMEM((streams * mem_slots, width), bf16),
            pltpu.VMEM(left_keys.shape, bf16),
            pltpu.VMEM(left_keys.shape, bf16),
            pltpu.VMEM((streams * mem_slots, cols), bf16),
            pltpu.VMEM((streams * mem_slots, cols), bf16),
            pltpu.VMEM((total, cols), f32),
            pltpu.VMEM((total, cols), f32),
            pltpu.VMEM((total, cols), f32),
            pltpu.VMEM((total, width), bf16),
            pltpu.VMEM((total, cols), f32),
            pltpu.VMEM((count, width), f32),
            pltpu.VMEM((count, width), bf16),
            pltpu.VMEM((count, width), bf16),
            pltpu.VMEM((count, n_ff * cols), bf16),
            pltpu.VMEM((count, n_ff * cols), bf16),
            pltpu.VMEM((count, width), f32),
            pltpu.VMEM((count, width), f32),
            pltpu.VMEM((count + streams, width), bf16),
            pltpu.VMEM((count + streams, width), bf16),
            pltpu.VMEM((4, count // 2, width), bf16),
            pltpu.VMEM((4, count // 2, width), bf16),
            pltpu.SemaphoreType.DMA((n_blocks, 6)),
            pltpu.SemaphoreType.DMA((n_blocks, 6)),
            pltpu.SemaphoreType.DMA((7,)),
            pltpu.SemaphoreType.DMA((7,)),
            pltpu.SemaphoreType.DMA((n_blocks + 7,)),
            pltpu.SemaphoreType.DMA((peers,)),
            pltpu.SemaphoreType.DMA((peers,)),
            pltpu.SemaphoreType.DMA((peers,)),
            pltpu.SemaphoreType.DMA((peers,)),
            pltpu.SemaphoreType.REGULAR((3,)),
        ],
        compiler_params=pltpu.CompilerParams(
            collective_id=0, has_side_effects=True, vmem_limit_bytes=60 * 1024 * 1024
        ),
    )(
        feed,
        memory_fill,
        left_length,
        out_gain.reshape(1, width),
        memory_bank.reshape(streams * mem_slots, width),
        left_keys,
        left_values,
        w_query,
        w_key,
        w_value,
        w_out,
        w_up,
        w_down,
    )
    layer_out, memory_next, center_keys, center_values = pl.pallas_call(
        finish,
        out_shape=tuple(jax.ShapeDtypeStruct(*r) for r in results),
        in_specs=[vmem] * 4,
        out_specs=(vmem,) * 4,
    )(*middle)
    layer_out = jnp.transpose(layer_out.reshape(frames, streams, width), (1, 0, 2))
    return (layer_out, memory_next, center_keys, center_values)


def solution(mesh):
    in_specs = (
        P(None, ("dp", "fsdp"), None),
        P(("dp", "fsdp"), None, None),
        P(("dp", "fsdp")),
        P(("dp", "fsdp"), None, "mp"),
        P(("dp", "fsdp"), None, "mp"),
        P(("dp", "fsdp")),
        P("fsdp", "mp"),
        P("fsdp", "mp"),
        P("fsdp", "mp"),
        P("mp", "fsdp"),
        P("fsdp", "mp"),
        P("mp", "fsdp"),
        P(),
    )
    out_specs = (
        P(("dp", "fsdp"), None, None),
        P(("dp", "fsdp"), None),
        P(("dp", "fsdp"), None, "mp"),
        P(("dp", "fsdp"), None, "mp"),
    )
    return jax.shard_map(shards, mesh=mesh, in_specs=in_specs, out_specs=out_specs, check_vma=False)
```

```python
import functools

import jax
import jax.numpy as jnp
from jax import lax
from jax.experimental import pallas as pl
from jax.experimental.pallas import tpu as pltpu
from jax.sharding import PartitionSpec as P

HD = 64
GROUP = 4
ROWS = 8
KEYS = 128
FIRST = 3
LEAD = 8
UNROLL = 8

epsilon = 1e-05
masked_score = -1e30
MESH = pl.DeviceIdType.MESH
bf16 = jnp.bfloat16
f32 = jnp.float32


def normalize(values):
    average = jnp.mean(values, axis=-1, keepdims=True)
    centred = values - average
    variance = jnp.mean(centred * centred, axis=-1, keepdims=True)
    return centred * lax.rsqrt(variance + epsilon)


def matmul(left, right):
    return jnp.dot(left, right, preferred_element_type=f32)


def body(
    frames,
    mem_slots,
    left_slots,
    packed,
    f_hbm,
    fill_hbm,
    length_hbm,
    gain_hbm,
    mem_hbm,
    lk_hbm,
    lv_hbm,
    wq_hbm,
    wk_hbm,
    wv_hbm,
    wo_hbm,
    wu_hbm,
    wd_hbm,
    out_hbm,
    mnext_hbm,
    ck_hbm,
    cv_hbm,
    mnext_ref,
    ck_ref,
    cv_ref,
    f_ref,
    fill_ref,
    length_ref,
    gain_ref,
    x_ref,
    outbox,
    inbox,
    far,
    own,
    mem_v,
    lk_v,
    lv_v,
    mk,
    mv,
    gk,
    gv,
    qs,
    s_buf,
    p_buf,
    rows_v,
    att,
    hid,
    hn,
    hn_far,
    act,
    act_far,
    dacc,
    dacc_far,
    part,
    peer,
    far_out,
    far_in,
    own_out,
    own_in,
    back_out,
    back_in,
    out_v,
    send_sem,
    recv_sem,
    psend_sem,
    precv_sem,
    load_sem,
    f_sem,
    hello,
    store_sem,
):
    d = lax.axis_index("dp")
    m = lax.axis_index("mp")
    f = lax.axis_index("fsdp")
    total, width = rows_v.shape
    streams = total // ROWS
    count = frames * streams
    half = count // 2
    n_blocks, depth, cols = far.shape
    n_ff = (n_blocks - 4) // 2
    n_hid = n_ff * cols
    quarter = depth // 4
    c1 = quarter // 4
    c2 = (quarter - c1) // 2
    ybit = lax.rem(d, 2)
    zbit = lax.rem(lax.div(d, 2), 2)
    p = lax.rem(d, 4)
    py = p + 1 - 2 * ybit
    pz = p + 2 - 4 * zbit
    pd = 3 - p
    xdev = (d, m, 1 - f)
    ydev = (d + 1 - 2 * ybit, m, f)
    zdev = (d + 2 - 4 * zbit, m, f)
    mdev = (d, 1 - m, f)

    part_cols = cols // 2
    ups = [4 + j for j in range(n_ff)]
    downs = [4 + n_ff + j for j in range(n_ff)]
    order = [(b, h) for b in (0, 1, 2, 3, *ups) for h in (0, 1)]
    order += [(b, h) for h in (0, 1) for b in downs]
    n_units = len(order)
    unit_of = {pair: u for u, pair in enumerate(order)}

    def own_hbm(u, start, size, side):
        b, h = order[u]
        shift = h * part_cols
        r = pl.ds(pl.multiple_of(start, 16), size)
        lanes = pl.ds(shift, part_cols)
        if b < 4:
            return (wq_hbm, wk_hbm, wv_hbm, wo_hbm)[b].at[r, lanes]
        if b in ups:
            first = side * n_hid + (b - ups[0]) * cols
            return wu_hbm.at[r, pl.ds(pl.multiple_of(first + shift, 128), part_cols)]
        first = side * n_hid + (b - downs[0]) * cols
        return wd_hbm.at[pl.ds(pl.multiple_of(start + first, 16), size), lanes]

    def own_block(b):
        if b < 4:
            return (wq_hbm, wk_hbm, wv_hbm, wo_hbm)[b]
        if b in ups:
            first = pl.multiple_of(f * n_hid + (b - ups[0]) * cols, 128)
            return wu_hbm.at[:, pl.ds(first, cols)]
        first = pl.multiple_of(f * n_hid + (b - downs[0]) * cols, 128)
        return wd_hbm.at[pl.ds(first, depth), :]

    def piece(u, start, size):
        b, h = order[u]
        lanes = pl.ds(h * part_cols, part_cols)
        return far.at[b, pl.ds(pl.multiple_of(start, 16), size), lanes]

    sends = []

    def remote(src, dst, s_sem, r_sem, dev):
        return pltpu.make_async_remote_copy(
            src_ref=src,
            dst_ref=dst,
            send_sem=s_sem,
            recv_sem=r_sem,
            device_id=dev,
            device_id_type=MESH,
        )

    def push(src, dst, i, dev):
        copy = remote(src, dst, psend_sem.at[i], precv_sem.at[i], dev)
        copy.start()
        sends.append(copy)

    def landed(ref, i):
        remote(ref, ref, psend_sem.at[i], precv_sem.at[i], xdev).wait_recv()

    def send(src, u, start, size, dev, kind):
        half_of = (2 * u) // n_units
        dst = piece(u, start, size)
        remote(src, dst, send_sem.at[half_of], recv_sem.at[u, kind], dev).start()

    def arrived(u, start, size, kind):
        ref = piece(u, start, size)
        remote(ref, ref, send_sem.at[0], recv_sem.at[u, kind], xdev).wait_recv()

    def load(src, dst, i):
        copy = pltpu.make_async_copy(src, dst, load_sem.at[i])
        copy.start()
        return copy

    n_fsdp = lax.axis_size("fsdp")
    me = d * n_fsdp + f
    wbit = lax.rem(lax.div(d, 4), 2)

    def across(mask):
        x, y, z, w = mask
        to_d = d + y * (1 - 2 * ybit) + 2 * z * (1 - 2 * zbit) + 4 * w * (1 - 2 * wbit)
        to_f = f + x * (1 - 2 * f)
        return (to_d, m, to_f), to_d * n_fsdp + to_f

    barrier = pltpu.get_barrier_semaphore()
    greeted = [xdev, ydev, zdev, mdev]
    if packed:
        greeted.append(across((0, 0, 0, 1))[0])
    for dev in greeted:
        pl.semaphore_signal(barrier, inc=1, device_id=dev, device_id_type=MESH)

    f_load = load(f_hbm, f_ref if packed else x_ref, n_blocks + 3)
    small_loads = [
        load(fill_hbm, fill_ref, n_blocks + 4),
        load(length_hbm, length_ref, n_blocks + 5),
        load(gain_hbm, gain_ref, n_blocks + 6),
    ]

    if packed:
        f_load.wait()
        pairs = outbox.shape[1]
        for k in range(pairs):
            low = f_ref[2 * k].astype(f32)
            high = f_ref[min(2 * k + 1, frames - 1)].astype(f32)
            turned = jnp.concatenate([low, high], axis=0).T.astype(bf16)
            outbox[:, k] = turned.reshape(outbox.shape[0], streams, turned.shape[1])

    with jax.named_scope("barwait"):
        pl.semaphore_wait(barrier, len(greeted))

    def send_own(u):
        if u >= n_units:
            return
        send(own_hbm(u, p * quarter, quarter, 1 - f), u, p * quarter, quarter, xdev, 0)
        send(own_hbm(u, pd * quarter, c1, 1 - f), u, pd * quarter, c1, xdev, 2)

    for u in range(FIRST):
        send_own(u)
    share = streams // 2

    def slot(box, i, side):
        return box.at[i, :, pl.ds(pl.multiple_of(side * share, 16), share), :]

    known = (
        ((1, 0, 0, 0), (0, 1, 0, 0), (0, 0, 1, 0), (0, 0, 0, 1)),
        ((1, 0, 1, 0), (0, 1, 1, 0), (0, 0, 1, 1)),
        ((1, 1, 0, 0), (0, 1, 0, 1), (0, 1, 1, 1), (1, 1, 1, 0)),
        ((1, 0, 0, 1), (1, 0, 1, 1), (1, 1, 0, 1), (1, 1, 1, 1)),
    )
    masks = [mask for group in known for mask in group]

    if packed:
        for i, group in enumerate(known):
            if i > 0:
                dev = (zdev, ydev, xdev)[i - 1]
                with jax.named_scope("hello%d" % i):
                    pl.semaphore_signal(
                        hello.at[i - 1], inc=1, device_id=dev, device_id_type=MESH
                    )
                    pl.semaphore_wait(hello.at[i - 1], 1)
            for mask in group:
                dev, index = across(mask)
                remote(
                    slot(outbox, index, m), slot(inbox, me, m), f_sem.at[0], f_sem.at[1], dev
                ).start()
    for u in range(FIRST, LEAD):
        send_own(u)

    loads = [load(own_block(b), own.at[b], b) for b in range(n_blocks)]
    mem_load = load(mem_hbm, mem_v, n_blocks)
    lk_load = load(lk_hbm, lk_v, n_blocks + 1)
    lv_load = load(lv_hbm, lv_v, n_blocks + 2)

    def pass_quarter(u):
        if u >= n_units:
            return
        arrived(u, p * quarter, quarter, 0)
        send_own(u + LEAD)
        src = piece(u, p * quarter, quarter)
        send(src, u, p * quarter, quarter, ydev, 1)
        send(src, u, p * quarter, quarter, zdev, 1)

    def pass_diagonal(u):
        if u < 0 or u >= n_units:
            return
        arrived(u, 0, 2 * quarter, 1)
        at_y = pz * quarter + c1
        send(piece(u, at_y, c2), u, at_y, c2, ydev, 2)
        at_z = py * quarter + c1 + c2
        send(piece(u, at_z, c2), u, at_z, c2, zdev, 2)

    def complete(u):
        arrived(u, pd * quarter, quarter, 2)
        if order[u][1] == 0 and order[u][0] not in downs:
            loads[order[u][0]].wait()

    pumped = [0]

    def pump(to):
        while pumped[0] <= to:
            u = pumped[0]
            with jax.named_scope("pump%d" % u):
                pass_diagonal(u - 2)
                pass_quarter(u)
            pumped[0] = u + 1

    mine = pl.ds(pl.multiple_of(f * depth, 128), depth)
    other = pl.ds(pl.multiple_of((1 - f) * depth, 128), depth)

    pump(3)

    others = inbox.at[pl.ds(0, max(inbox.shape[0] - 1, 1)), :, pl.ds(0, share), :]

    def features_in():
        inbox[pl.ds(me, 1)] = outbox[pl.ds(me, 1)]
        with jax.named_scope("fwait"):
            remote(others, others, f_sem.at[0], f_sem.at[1], xdev).wait_recv()
        for mask in masks:
            ref = slot(inbox, across(mask)[1], m)
            remote(ref, ref, f_sem.at[2], f_sem.at[3], mdev).start()

    def features_out():
        with jax.named_scope("gwait"):
            remote(others, others, f_sem.at[2], f_sem.at[3], xdev).wait_recv()
        lane_half = inbox.shape[3] // 2
        for t in range(frames):
            k, side = t // 2, t % 2
            lanes = slice(side * lane_half, side * lane_half + lane_half)
            x_ref[t * streams : (t + 1) * streams, :] = jnp.concatenate(
                [inbox[i, k][:, lanes] for i in range(inbox.shape[0])], axis=1
            )

    packed_rows = count + streams

    def normalize_rows():
        summed = None
        major = []
        for t in range(frames):
            n = normalize(x_ref[t * streams : (t + 1) * streams, :].astype(f32)).astype(bf16)
            major.append(n)
            if t < GROUP:
                summed = n.astype(f32) if t == 0 else summed + n.astype(f32)
        major.append((summed * (1.0 / GROUP)).astype(bf16))
        major = jnp.concatenate(major, axis=0)
        r_id = lax.broadcasted_iota(jnp.int32, (total, packed_rows), 0)
        c_id = lax.broadcasted_iota(jnp.int32, (total, packed_rows), 1)
        frame_id = r_id % ROWS
        target = jnp.where(frame_id <= frames, frame_id * streams + r_id // ROWS, -1)
        spread_rows = jnp.where(target == c_id, 1.0, 0.0).astype(bf16)
        rows_v[...] = matmul(spread_rows, major).astype(bf16)

    def lanes_of(h):
        return slice(h * part_cols, (h + 1) * part_cols)

    def project(b, h):
        sums = matmul(rows_v[:, mine], own[b, :, lanes_of(h)])
        sums = sums + matmul(rows_v[:, other], far[b, :, lanes_of(h)])
        return sums.astype(bf16).astype(f32)

    def project_memory(b, h, target):
        step = 512

        @pl.loop(0, mem_v.shape[0] // step)
        def _(i):
            r = pl.ds(pl.multiple_of(i * step, step), step)
            sums = matmul(mem_v[r, mine], own[b, :, lanes_of(h)])
            sums = sums + matmul(mem_v[r, other], far[b, :, lanes_of(h)])
            target[r, lanes_of(h)] = sums.astype(bf16)

    def await_unit(b, h):
        u = unit_of[b, h]
        pump(max(u + 2, min(u + 3, 5)))
        with jax.named_scope("c%d" % u):
            complete(u)

    def store(src, dst, i):
        copy = pltpu.make_async_copy(src, dst, store_sem.at[i])
        copy.start()
        return copy

    def project_group(b, h, target, kept):
        values = project(b, h).reshape(streams, ROWS, part_cols)
        kept[:, :, lanes_of(h)] = values[:, :GROUP].astype(bf16)
        padded = jnp.concatenate([values, jnp.zeros_like(values)], axis=1)
        target[:, lanes_of(h)] = padded.reshape(2 * total, part_cols).astype(bf16)

    heads = part_cols // HD
    span = heads * ROWS
    lanes3 = lax.broadcasted_iota(jnp.int32, (heads, ROWS, part_cols), 2)
    head3 = lax.broadcasted_iota(jnp.int32, (heads, ROWS, part_cols), 0)
    head_mask = jnp.where(lanes3 // HD == head3, 1.0, 0.0).astype(f32)
    row2 = lax.broadcasted_iota(jnp.int32, (span, KEYS), 0)
    lane2 = lax.broadcasted_iota(jnp.int32, (span, KEYS), 1)
    excluded = jnp.where((row2 % ROWS == frames) & (lane2 < mem_slots), -1.0, 0.0).astype(f32)
    lane1 = lax.broadcasted_iota(jnp.int32, (1, KEYS), 1)
    left_end = mem_slots + left_slots
    pad = jnp.zeros((KEYS - mem_slots - left_slots - 2 * ROWS, part_cols), bf16)
    scale = HD ** (-0.5)

    def gather_rows(mem_part, left_part, group_part, s, h):
        return jnp.concatenate(
            [
                mem_part[pl.ds(pl.multiple_of(s * mem_slots, mem_slots), mem_slots), lanes_of(h)],
                left_part[s, :, lanes_of(h)],
                group_part[pl.ds(pl.multiple_of(s * 2 * ROWS, 2 * ROWS), 2 * ROWS), lanes_of(h)],
                pad,
            ],
            axis=0,
        )

    def stream_rows(s):
        return pl.ds(pl.multiple_of(s * ROWS, ROWS), ROWS)

    def score_rows(s):
        return pl.ds(pl.multiple_of(s * span, span), span)

    def score(s, h):
        spread = (qs[stream_rows(s), lanes_of(h)][None] * head_mask).reshape(span, part_cols)
        k = gather_rows(mk, lk_v, gk, s, h)
        scores = lax.dot_general(
            spread.astype(bf16), k, (((1,), (1,)), ((), ())), preferred_element_type=f32
        )
        first_mem = mem_slots - fill_ref[s]
        first_left = left_end - length_ref[s]
        first = jnp.where(lane1 < mem_slots, first_mem, first_left)
        first = jnp.where(lane1 < left_end, first, 0)
        hide1 = (lane1 < first) | (lane1 >= left_end + frames)
        hide = jnp.where(hide1, -1.0, 0.0) + excluded
        s_buf[score_rows(s), :] = jnp.where(hide < 0.0, masked_score, scores * scale)

    def soften(h):
        step = 256

        @pl.loop(0, s_buf.shape[0] // step)
        def _(i):
            r = pl.ds(pl.multiple_of(i * step, step), step)
            scores = s_buf[r, :]
            e = jnp.exp(scores - jnp.max(scores, axis=-1, keepdims=True))
            p_buf[h, r, :] = (e / jnp.sum(e, axis=-1, keepdims=True)).astype(bf16)

    def combine(s, h):
        v = gather_rows(mv, lv_v, gv, s, h)
        o = matmul(p_buf[h, score_rows(s), :], v).reshape(heads, ROWS, part_cols) * head_mask
        att[stream_rows(s), lanes_of(h)] = jnp.sum(o, axis=0)

    def each_stream(do, h):
        @pl.loop(0, streams // UNROLL)
        def _(i):
            for t in range(UNROLL):
                do(i * UNROLL + t, h)

    if packed:
        features_in()
    else:
        f_load.wait()
    await_unit(0, 0)
    if packed:
        features_out()
    with jax.named_scope("norm"):
        normalize_rows()
    with jax.named_scope("q0"):
        qs[:, lanes_of(0)] = project(0, 0)
    await_unit(0, 1)
    with jax.named_scope("q1"):
        qs[:, lanes_of(1)] = project(0, 1)
    for copy in [mem_load, lk_load, lv_load] + small_loads:
        copy.wait()
    for h in (0, 1):
        await_unit(1, h)
        with jax.named_scope("mk%d" % h):
            project_memory(1, h, mk)
        pump(6 + 2 * h)
        with jax.named_scope("gk%d" % h):
            project_group(1, h, gk, ck_ref)
        with jax.named_scope("score%d" % h):
            each_stream(score, h)
        pump(7 + 2 * h)
        with jax.named_scope("soft%d" % h):
            soften(h)
    stores = [store(ck_ref, ck_hbm, 0)]
    for h in (0, 1):
        await_unit(2, h)
        with jax.named_scope("mv%d" % h):
            project_memory(2, h, mv)
        pump(10 + h)
        with jax.named_scope("gv%d" % h):
            project_group(2, h, gv, cv_ref)
        with jax.named_scope("comb%d" % h):
            each_stream(combine, h)
    stores.append(store(cv_ref, cv_hbm, 1))

    def both(b):
        await_unit(b, 0)
        await_unit(b, 1)

    both(3)
    with jax.named_scope("oproj"):
        r_id = lax.broadcasted_iota(jnp.int32, (packed_rows, total), 0)
        c_id = lax.broadcasted_iota(jnp.int32, (packed_rows, total), 1)
        pick = (r_id % streams) * ROWS + r_id // streams
        gather = jnp.where(pick == c_id, 1.0, 0.0).astype(bf16)
        attended = matmul(gather, att[...].astype(bf16)).astype(bf16)
        part[:, mine] = matmul(attended, own[3]).astype(bf16)
        part[:, other] = matmul(attended, far[3]).astype(bf16)
    push(part, peer, 0, mdev)
    pump(12)
    with jax.named_scope("ex0"):
        landed(peer, 0)

    my_half = pl.multiple_of(m * half, 16)
    its_half = pl.multiple_of((1 - m) * half, 16)
    rows_mine = pl.ds(my_half, half)
    rows_its = pl.ds(its_half, half)

    def residual(r):
        h = x_ref[r, :].astype(f32) + (part[r, :].astype(f32) + peer[r, :].astype(f32))
        hid[r, :] = h
        hn[r, :] = normalize(h).astype(bf16)

    with jax.named_scope("hid"):
        residual(rows_mine)
        push(hn.at[rows_mine, :], hn_far.at[rows_mine, :], 1, xdev)
        pump(13)
        residual(rows_its)
        s = slice(count, packed_rows)
        mnext_ref[...] = jnp.tanh(part[s, :].astype(f32) + peer[s, :].astype(f32)).astype(bf16)
        stores.append(store(mnext_ref, mnext_hbm, 2))

    def up(rows, target, j):
        sums = matmul(rows[:, mine], own[ups[j]]) + matmul(rows[:, other], far[ups[j]])
        target[:, j * cols : (j + 1) * cols] = jax.nn.gelu(sums, approximate=True).astype(bf16)

    def down(rows, weights, lanes):
        sums = None
        for j in range(n_ff):
            term = matmul(rows[:, j * cols : (j + 1) * cols], weights[downs[j], :, lanes])
            sums = term if sums is None else sums + term
        return sums

    pump(14)
    for j in range(n_ff):
        both(ups[j])
        with jax.named_scope("up%d" % j):
            up(hn, act, j)
        pump(15 + j)
    with jax.named_scope("hnwait"):
        landed(hn_far.at[rows_mine, :], 1)
        push(hn_far.at[rows_mine, :], hn_far.at[rows_mine, :], 2, mdev)
        landed(hn_far.at[rows_its, :], 2)
    with jax.named_scope("farup"):
        for j in range(n_ff):
            up(hn_far, act_far, j)
    pump(n_units + 1)

    shift = pl.multiple_of((1 - f) * depth, 128)
    spans = [(own, slice(0, cols), mine)]
    for h in (0, 1):
        spans.append((far, lanes_of(h), pl.ds(shift + h * part_cols, part_cols)))

    for b in downs:
        loads[b].wait()
    for i, (weights, lanes, dst) in enumerate(spans):
        if i > 0:
            for b in downs:
                await_unit(b, i - 1)
        with jax.named_scope("fardn%d" % i):
            sums = down(act_far, weights, lanes)
            dacc_far[:, dst] = sums
            far_out[rows_its, dst] = dacc_far[rows_its, dst].astype(bf16)
        push(far_out.at[rows_its, dst], far_in.at[rows_its, dst], 3 + 2 * i, mdev)
        with jax.named_scope("owndn%d" % i):
            dacc[:, dst] = down(act, weights, lanes)
            own_out[:, dst] = dacc[:, dst].astype(bf16)
        if i == len(spans) - 1:
            push(own_out, own_in, 9, mdev)
        with jax.named_scope("xsum%d" % i):
            landed(far_in.at[rows_mine, dst], 3 + 2 * i)
            both_sums = dacc_far[rows_mine, dst] + far_in[rows_mine, dst].astype(f32)
            back_out[:, dst] = both_sums.astype(bf16)
        push(back_out.at[:, dst], back_in.at[:, dst], 4 + 2 * i, xdev)
    with jax.named_scope("ownsum"):
        landed(own_in, 9)
        y = hid[rows_mine, :] + (dacc[rows_mine, :] + own_in[rows_mine, :].astype(f32))
        hid[rows_mine, :] = y
    with jax.named_scope("xwait"):
        for i, (_, _, dst) in enumerate(spans):
            landed(back_in.at[:, dst], 4 + 2 * i)
    with jax.named_scope("final"):
        y = hid[rows_mine, :] + back_in[...].astype(f32)
        out_v[rows_mine, :] = (normalize(y) * gain_ref[...]).astype(bf16)
    push(out_v.at[rows_mine, :], out_v.at[rows_mine, :], 10, mdev)
    stores.append(store(out_v.at[rows_mine, :], out_hbm.at[rows_mine, :], 3))
    with jax.named_scope("lastwait"):
        landed(out_v.at[rows_its, :], 10)
    stores.append(store(out_v.at[rows_its, :], out_hbm.at[rows_its, :], 4))

    with jax.named_scope("sendwait"):
        for copy in sends:
            copy.wait_send()
        for i in range(2):
            ref = far.at[pl.ds(i * (n_blocks // 2), n_blocks // 2), :, :]
            remote(ref, ref, send_sem.at[i], recv_sem.at[0, 0], xdev).wait_send()
        if packed:
            for i in (0, 2):
                remote(others, others, f_sem.at[i], f_sem.at[1], xdev).wait_send()
        for copy in stores:
            copy.wait()


def finish(rows_hbm, mem_hbm, keys_hbm, vals_hbm, out_hbm, mnext_hbm, ck_hbm, cv_hbm, *scratch):
    buffers, (in_sem, out_sem) = scratch[:4], scratch[4:]
    arrays = (
        (rows_hbm, buffers[0], out_hbm),
        (mem_hbm, buffers[1], mnext_hbm),
        (keys_hbm, buffers[2], ck_hbm),
        (vals_hbm, buffers[3], cv_hbm),
    )
    ins = [pltpu.make_async_copy(a, b, in_sem.at[i]) for i, (a, b, _) in enumerate(arrays)]
    outs = [pltpu.make_async_copy(b, c, out_sem.at[i]) for i, (_, b, c) in enumerate(arrays)]
    for copy in ins:
        copy.start()
    for first, second in zip(ins, outs):
        first.wait()
        second.start()
    for copy in outs:
        copy.wait()


def shards(
    features,
    memory_bank,
    memory_fill,
    left_keys,
    left_values,
    left_length,
    w_query,
    w_key,
    w_value,
    w_out,
    w_up,
    w_down,
    out_gain,
):
    frames, width_dev, all_streams = features.shape
    streams, mem_slots, width = memory_bank.shape
    left_slots = left_keys.shape[1]
    depth, cols = w_query.shape
    n_dp = lax.axis_size("dp")
    n_fsdp = lax.axis_size("fsdp")
    n_ff = w_up.shape[1] // (n_fsdp * cols)
    n_blocks = 4 + 2 * n_ff
    total = streams * ROWS
    count = frames * streams
    peers = n_dp * n_fsdp
    packed = 2 * width_dev == KEYS and streams % 32 == 0 and n_dp == 8 and n_fsdp == 2
    if packed:
        feed = features
    else:
        flat = features.reshape(frames * width_dev, all_streams)
        got = lax.all_to_all(flat, ("dp", "fsdp"), split_axis=1, concat_axis=0, tiled=True)
        got = got.reshape(peers, frames, width_dev, streams)
        feed = jnp.transpose(got, (1, 3, 0, 2)).reshape(count, width)
    slots = (peers, (frames + 1) // 2, streams, KEYS) if packed else (1, 1, 32, KEYS)
    hbm = pl.BlockSpec(memory_space=pl.ANY)
    results = (
        ((count, width), bf16),
        ((streams, width), bf16),
        ((streams, GROUP, cols), bf16),
        ((streams, GROUP, cols), bf16),
    )
    middle = pl.pallas_call(
        functools.partial(body, frames, mem_slots, left_slots, packed),
        out_shape=tuple(jax.ShapeDtypeStruct(*r) for r in results),
        in_specs=[hbm] * 13,
        out_specs=(hbm,) * 4,
        scratch_shapes=[pltpu.VMEM(*r) for r in results[1:]]
        + [
            pltpu.VMEM(features.shape if packed else (1, 16, KEYS), bf16),
            pltpu.SMEM((streams,), jnp.int32),
            pltpu.SMEM((streams,), jnp.int32),
            pltpu.VMEM((1, width), f32),
            pltpu.VMEM((count, width), bf16),
            pltpu.VMEM(slots, bf16),
            pltpu.VMEM(slots, bf16),
            pltpu.VMEM((n_blocks, depth, cols), bf16),
            pltpu.VMEM((n_blocks, depth, cols), bf16),
            pltpu.VMEM((streams * mem_slots, width), bf16),
            pltpu.VMEM(left_keys.shape, bf16),
            pltpu.VMEM(left_keys.shape, bf16),
            pltpu.VMEM((streams * mem_slots, cols), bf16),
            pltpu.VMEM((streams * mem_slots, cols), bf16),
            pltpu.VMEM((2 * total, cols), bf16),
            pltpu.VMEM((2 * total, cols), bf16),
            pltpu.VMEM((total, cols), f32),
            pltpu.VMEM((streams * ROWS * cols // (2 * HD), KEYS), f32),
            pltpu.VMEM((2, streams * ROWS * cols // (2 * HD), KEYS), bf16),
            pltpu.VMEM((total, width), bf16),
            pltpu.VMEM((total, cols), f32),
            pltpu.VMEM((count, width), f32),
            pltpu.VMEM((count, width), bf16),
            pltpu.VMEM((count, width), bf16),
            pltpu.VMEM((count, n_ff * cols), bf16),
            pltpu.VMEM((count, n_ff * cols), bf16),
            pltpu.VMEM((count, width), f32),
            pltpu.VMEM((count, width), f32),
            pltpu.VMEM((count + streams, width), bf16),
            pltpu.VMEM((count + streams, width), bf16),
            pltpu.VMEM((count, width), bf16),
            pltpu.VMEM((count, width), bf16),
            pltpu.VMEM((count, width), bf16),
            pltpu.VMEM((count, width), bf16),
            pltpu.VMEM((count // 2, width), bf16),
            pltpu.VMEM((count // 2, width), bf16),
            pltpu.VMEM((count, width), bf16),
            pltpu.SemaphoreType.DMA((2,)),
            pltpu.SemaphoreType.DMA((2 * n_blocks, 3)),
            pltpu.SemaphoreType.DMA((11,)),
            pltpu.SemaphoreType.DMA((11,)),
            pltpu.SemaphoreType.DMA((n_blocks + 7,)),
            pltpu.SemaphoreType.DMA((4,)),
            pltpu.SemaphoreType.REGULAR((3,)),
            pltpu.SemaphoreType.DMA((5,)),
        ],
        compiler_params=pltpu.CompilerParams(
            collective_id=0, has_side_effects=True, vmem_limit_bytes=60 * 1024 * 1024
        ),
    )(
        feed,
        memory_fill,
        left_length,
        out_gain.reshape(1, width),
        memory_bank.reshape(streams * mem_slots, width),
        left_keys,
        left_values,
        w_query,
        w_key,
        w_value,
        w_out,
        w_up,
        w_down,
    )
    layer_out, memory_next, center_keys, center_values = pl.pallas_call(
        finish,
        out_shape=tuple(jax.ShapeDtypeStruct(*r) for r in results),
        in_specs=[hbm] * 4,
        out_specs=(hbm,) * 4,
        scratch_shapes=[pltpu.VMEM(*r) for r in results] + [pltpu.SemaphoreType.DMA((4,))] * 2,
        compiler_params=pltpu.CompilerParams(vmem_limit_bytes=60 * 1024 * 1024),
    )(*middle)
    layer_out = jnp.transpose(layer_out.reshape(frames, streams, width), (1, 0, 2))
    return (layer_out, memory_next, center_keys, center_values)


def solution(mesh):
    in_specs = (
        P(None, ("dp", "fsdp"), None),
        P(("dp", "fsdp"), None, None),
        P(("dp", "fsdp")),
        P(("dp", "fsdp"), None, "mp"),
        P(("dp", "fsdp"), None, "mp"),
        P(("dp", "fsdp")),
        P("fsdp", "mp"),
        P("fsdp", "mp"),
        P("fsdp", "mp"),
        P("mp", "fsdp"),
        P("fsdp", "mp"),
        P("mp", "fsdp"),
        P(),
    )
    out_specs = (
        P(("dp", "fsdp"), None, None),
        P(("dp", "fsdp"), None),
        P(("dp", "fsdp"), None, "mp"),
        P(("dp", "fsdp"), None, "mp"),
    )
    return jax.shard_map(shards, mesh=mesh, in_specs=in_specs, out_specs=out_specs, check_vma=False)
```
